32 devices in a mesh: dp: 4 (over z), seq: 4 (over y, core), tp: 2 (over x).
Axes of the slice: x: 2, y: 2, z: 4, core: 2. Of those that a mesh axis runs over, the one named last changes fastest.
Arguments:
- queries: bfloat16 [8192, 1024], P(('dp', 'seq'), 'tp'), parts along dimension 0, may hold values from -181 to 181
- rotated_key_states: bfloat16 [8192, 256], P(('dp', 'seq'), 'tp'), parts along dimension 0, may hold values from -6.1 to 6.1
- value_state_vectors: bfloat16 [8192, 256], P(('dp', 'seq'), 'tp'), parts along dimension 0, may hold values from -6 to 6
- out_weight: bfloat16 [1024, 8192], P('tp'), may hold values from -0.3125 to 0.3125
- residual: bfloat16 [8192, 8192], P(('dp', 'seq', 'tp')), parts along dimension 0, may hold values from -0.75 to 0.75
- norm_gain: bfloat16 [8192], replicated, may hold values from 0.099609375 to 2
Outputs:
- new_residual: bfloat16 [8192, 8192], P(('dp', 'seq', 'tp')), parts along dimension 0
- next_input: bfloat16 [8192, 8192], P(('dp', 'seq', 'tp')), parts along dimension 0
The draws below stay inside these ranges and needn't reach their ends.
There are 4 independent parts, one for each index of `dp`. The reference program is written for one: setup_inputs(seed, part) draws one part's arguments, and reference() takes and returns one part's arrays. A program takes and returns all parts, laid end to end along the dimension named above; an argument that names none is the same for every part. Nothing has to cross between parts.
All inputs are finite; a program needn't handle non-finite values.
Results may differ from the reference program's by a relative error of at most 0.025.
Values may be sent and summed in bfloat16 or wider, within the bound.
No kernel may reach another device: no remote copies, remote signals or barrier semaphores. Data moves between devices by JAX's collectives and lax.ppermute only.
A program may use at most 192 MiB of HBM per device.

```python
import math
import jax
import jax.numpy as jnp
from jax import lax

D = 8192
HEAD_SIZE = 128
HQ_DEV = 4
QUERY_HEADS = 8
KEY_VALUE_HEADS = 2
SEQUENCE_TOKENS = 2048
N_TP = 2


def drawn_pair(key):
    query_key = jax.random.fold_in(key, 11)
    random_key_for_keys = jax.random.fold_in(key, 12)
    query_rows = 1.2 * jnp.clip(jax.random.normal(query_key, (SEQUENCE_TOKENS, QUERY_HEADS * HEAD_SIZE), jnp.float32), -5.0, 5.0)
    key_row_block = 1.2 * jnp.clip(jax.random.normal(random_key_for_keys, (SEQUENCE_TOKENS, KEY_VALUE_HEADS * HEAD_SIZE), jnp.float32), -5.0, 5.0)
    return (query_rows, key_row_block)


def draw_queries(key, part):
    return drawn_pair(key)[0].astype(jnp.bfloat16)


def draw_rotated_key_states(key, part):
    return drawn_pair(key)[1].astype(jnp.bfloat16)


def draw_out_weight(key, part):
    row_total = QUERY_HEADS * HEAD_SIZE
    entry_key = jax.random.fold_in(key, 31)
    factor_key = jax.random.fold_in(key, 32)
    entries = jnp.clip(jax.random.normal(entry_key, (row_total // 16, 16, D), jnp.float32), -5.0, 5.0)
    exponents = jax.random.uniform(factor_key, (row_total // 16, 1, D), jnp.float32, jnp.log(1.0 / 16.0), 0.0)
    factors = jnp.exp(exponents)
    group_count = QUERY_HEADS // HQ_DEV
    block_index = jnp.arange(row_total // 16, dtype=jnp.int32)
    group_index = block_index * 16 // (HQ_DEV * HEAD_SIZE)
    group_frac = group_index.astype(jnp.float32) / max(group_count - 1, 1)
    group_scale = jnp.exp(jnp.log(4.0) * (group_frac - 1.0)).reshape(row_total // 16, 1, 1)
    scaled = entries * factors * group_scale * (2.0 / row_total ** 0.5)
    return scaled.reshape(row_total, D).astype(jnp.bfloat16)


def block_levels(own_key, shape, cuts, low, top_value):
    loudness, own = 1.0, jax.random.fold_in(own_key, 6)
    for dim, shards_of in cuts:
        heights = jnp.exp(jax.random.uniform(jax.random.fold_in(own, dim), (shards_of,), jnp.float32, low / len(cuts), top_value / len(cuts)))
        loudness = loudness * jnp.repeat(heights, shape[dim] // shards_of).reshape([-1 if axis == dim else 1 for axis in range(len(shape))])
    return loudness


def gaussian(own_key, extent, scale, reach, cuts=(), kind=jnp.bfloat16):
    level = block_levels(own_key, extent, cuts, -0.22, 0.18) if cuts else 1.0
    array = jax.random.normal(own_key, extent, jnp.float32) * scale * level
    return jnp.minimum(jnp.maximum(array, -reach), reach).astype(kind)


def setup_inputs(seed: int = 0, part: int = 0) -> dict:
    arg_keys = jax.random.split(jax.random.key(seed), 7)
    own_keys = jax.random.split(jax.random.fold_in(arg_keys[6], part), 7)
    return {
        "queries": draw_queries(jax.random.fold_in(jax.random.fold_in(arg_keys[6], part), 71), part),
        "rotated_key_states": draw_rotated_key_states(jax.random.fold_in(jax.random.fold_in(arg_keys[6], part), 71), part),
        "value_state_vectors": gaussian(own_keys[2], (SEQUENCE_TOKENS, KEY_VALUE_HEADS * HEAD_SIZE), 1.0, 6.0, ((0, 4), (1, 2))),
        "out_weight": draw_out_weight(jax.random.fold_in(arg_keys[6], 71), part),
        "residual": gaussian(own_keys[4], (SEQUENCE_TOKENS, D), 0.05, 0.75, ((0, 8),)),
        "norm_gain": jnp.clip(jnp.exp(jax.random.uniform(arg_keys[5], (D,), jnp.float32, math.log(0.099609375), math.log(2.0))), 0.099609375, 2.0).astype(jnp.bfloat16),
    }


softness = 0.9
scale_floor = 256.0

def soft_grid(values):
    return values - softness * jnp.sin(jnp.pi * values) / jnp.pi

def fake_quant(blocks, block_axis, peak):
    block_max = lax.optimization_barrier(jnp.max(jnp.abs(blocks), axis=block_axis, keepdims=True))
    tensor_scale = peak / (6.0 * 448.0)
    block_scale = jnp.maximum(block_max / (6.0 * tensor_scale), scale_floor).astype(jnp.bfloat16)
    block_scale = lax.optimization_barrier(block_scale).astype(jnp.float32)
    spacing = block_scale * tensor_scale
    payload = soft_grid(blocks / spacing).astype(jnp.bfloat16)
    payload = lax.optimization_barrier(payload).astype(jnp.float32)
    return (payload * spacing).astype(jnp.bfloat16)

def reference(queries, rotated_key_states, value_state_vectors, out_weight, residual, norm_gain):
    score_scale = HEAD_SIZE ** (-0.5)
    grouped_heads = QUERY_HEADS // KEY_VALUE_HEADS
    q_heads = queries.reshape(SEQUENCE_TOKENS, QUERY_HEADS, HEAD_SIZE)
    key_heads = rotated_key_states.reshape(SEQUENCE_TOKENS, KEY_VALUE_HEADS, HEAD_SIZE)
    value_heads = value_state_vectors.reshape(SEQUENCE_TOKENS, KEY_VALUE_HEADS, HEAD_SIZE)
    positions = jnp.arange(SEQUENCE_TOKENS, dtype=jnp.int32)
    allowed = positions[:, None] >= positions[None, :]

    def one_head(head_index):
        q_one = lax.dynamic_index_in_dim(q_heads, head_index, 1, keepdims=False)
        kv_index = head_index // grouped_heads
        k_one = lax.dynamic_index_in_dim(key_heads, kv_index, 1, keepdims=False)
        v_one = lax.dynamic_index_in_dim(value_heads, kv_index, 1, keepdims=False)
        scores = jnp.dot(q_one, k_one.T, preferred_element_type=jnp.float32) * score_scale
        scores = jnp.where(allowed, scores, -jnp.inf)
        row_top = lax.optimization_barrier(jnp.max(scores, axis=1, keepdims=True))
        weights = jnp.exp(scores - row_top)
        totals = lax.optimization_barrier(jnp.sum(weights, axis=1, keepdims=True))
        attended = jnp.dot(weights.astype(jnp.bfloat16), v_one, preferred_element_type=jnp.float32) / totals
        return attended.astype(jnp.bfloat16)
    attended = lax.map(one_head, jnp.arange(QUERY_HEADS, dtype=jnp.int32))
    features = QUERY_HEADS * HEAD_SIZE
    act_t = attended.transpose(0, 2, 1).reshape(features, SEQUENCE_TOKENS).astype(jnp.float32)
    act_peak = jnp.max(jnp.abs(act_t))
    act_q = fake_quant(act_t.reshape(features // 16, 16, SEQUENCE_TOKENS), 1, act_peak).reshape(features, SEQUENCE_TOKENS)
    weight_f = out_weight.astype(jnp.float32)
    weight_peak = jnp.max(jnp.abs(weight_f))
    weight_q = fake_quant(weight_f.reshape(features // 16, 16, D), 1, weight_peak).reshape(features, D)
    group_width = features // N_TP
    projected = jnp.zeros((SEQUENCE_TOKENS, D), jnp.float32)
    for group_rank in range(N_TP):
        lower = group_rank * group_width
        partial_sum = lax.dot_general(act_q[lower:lower + group_width], weight_q[lower:lower + group_width], (((0,), (0,)), ((), ())), preferred_element_type=jnp.float32)
        partial_sum = lax.optimization_barrier(partial_sum.astype(jnp.bfloat16)).astype(jnp.float32)
        projected = projected + partial_sum
    hidden_sum = residual.astype(jnp.float32) + projected
    new_residual = hidden_sum.astype(jnp.bfloat16)
    mean_square = lax.optimization_barrier(jnp.mean(hidden_sum * hidden_sum, axis=1, keepdims=True))
    normed = hidden_sum * lax.rsqrt(mean_square + 1e-05) * norm_gain.astype(jnp.float32)
    norm_peak = jnp.max(jnp.abs(normed))
    next_input = fake_quant(normed.reshape(SEQUENCE_TOKENS, D // 16, 16), 2, norm_peak).reshape(SEQUENCE_TOKENS, D)
    return (new_residual, next_input)
```

```python
import functools
import math

import jax
import jax.numpy as jnp
from jax import lax
from jax.experimental import pallas as pl
from jax.experimental.pallas import tpu as pltpu
from jax.sharding import PartitionSpec as P

D = 8192
HEAD_SIZE = 128


softness = 0.9
scale_floor = 256.0
neg_large = -1e30

def soft_grid(values):
    return values - softness * jnp.sin(jnp.pi * values) / jnp.pi


def fake_quant(blocks, block_axis, peak):
    block_max = jnp.max(jnp.abs(blocks), axis=block_axis, keepdims=True)
    tensor_scale = peak / (6.0 * 448.0)
    block_scale = jnp.maximum(block_max / (6.0 * tensor_scale), scale_floor).astype(jnp.bfloat16)
    block_scale = lax.optimization_barrier(block_scale).astype(jnp.float32)
    spacing = block_scale * tensor_scale
    payload = soft_grid(blocks / spacing).astype(jnp.bfloat16)
    payload = lax.optimization_barrier(payload).astype(jnp.float32)
    return (payload * spacing).astype(jnp.bfloat16)


def attend_piece(attn_state, q_grouped, kv_piece, query_pos, causal_piece):
    running_max, running_total, running_sum = attn_state
    kv_heads = q_grouped.shape[1]
    piece_rows = kv_piece.shape[1]
    keys_split = kv_piece[0].reshape(piece_rows, kv_heads, HEAD_SIZE)
    values_split = kv_piece[1].reshape(piece_rows, kv_heads, HEAD_SIZE)
    scores = jnp.einsum(
        "tkgd,skd->kgts", q_grouped, keys_split, preferred_element_type=jnp.float32
    ) * HEAD_SIZE ** (-0.5)
    if causal_piece:
        key_pos = lax.broadcasted_iota(jnp.int32, (1, piece_rows), 1)
        allowed = query_pos[:, None] >= key_pos
        masked = jnp.where(allowed, scores, neg_large)
        new_max = jnp.maximum(running_max, jnp.max(masked, axis=3))
        weights = jnp.where(allowed, jnp.exp(masked - new_max[..., None]), 0.0)
    else:
        new_max = jnp.maximum(running_max, jnp.max(scores, axis=3))
        weights = jnp.exp(scores - new_max[..., None])
    shrink_factor = jnp.exp(running_max - new_max)
    running_total = running_total * shrink_factor + jnp.sum(weights, axis=3)
    running_sum = running_sum * shrink_factor[..., None] + jnp.einsum(
        "kgts,skd->kgtd",
        weights.astype(jnp.bfloat16),
        values_split,
        preferred_element_type=jnp.float32,
    )
    return (new_max, running_total, running_sum)


def scatter_local(queries, rotated_key_states, value_state_vectors, out_weight, residual, norm_gain):
    token_count = queries.shape[0]
    kv_heads = rotated_key_states.shape[1] // HEAD_SIZE
    grouped_heads = queries.shape[1] // HEAD_SIZE // kv_heads
    seq_rank = lax.axis_index("seq")
    q_grouped = queries.reshape(token_count, kv_heads, grouped_heads, HEAD_SIZE)
    first_query = seq_rank * token_count
    last_query = first_query + token_count - 1
    query_pos = first_query + lax.broadcasted_iota(jnp.int32, (token_count,), 0)
    kv_own = jnp.stack((rotated_key_states, value_state_vectors))
    start_state = (
        jnp.full((kv_heads, grouped_heads, token_count), neg_large, jnp.float32),
        jnp.zeros((kv_heads, grouped_heads, token_count), jnp.float32),
        jnp.zeros((kv_heads, grouped_heads, token_count, HEAD_SIZE), jnp.float32),
    )

    def fold_piece(attn_state, kv_piece, first_row):
        piece_rows = kv_piece.shape[1]

        def before_queries(state_in):
            return attend_piece(state_in, q_grouped, kv_piece, query_pos, False)

        def across_queries(state_in):
            return attend_piece(state_in, q_grouped, kv_piece, query_pos, True)

        def after_queries(state_in):
            return state_in

        branch_index = jnp.where(
            first_row + piece_rows <= first_query, 0, jnp.where(first_row <= last_query, 1, 2)
        ).astype(jnp.int32)
        return lax.switch(branch_index, [before_queries, across_queries, after_queries], attn_state)

    final_state = fold_piece(
        start_state, lax.all_gather(kv_own, "seq", axis=1, tiled=True), jnp.int32(0)
    )
    attended = (final_state[2] / final_state[1][..., None]).astype(jnp.bfloat16)
    features = attended.shape[0] * attended.shape[1] * HEAD_SIZE
    act_t = attended.transpose(0, 1, 3, 2).reshape(features, token_count).astype(jnp.float32)
    weight_f = out_weight.astype(jnp.float32)
    act_local = jnp.max(jnp.abs(act_t))
    weight_local = jnp.max(jnp.abs(weight_f))
    weight_peak = lax.pmax(weight_local, "tp")
    act_peak = lax.pmax(act_local, ("seq", "tp"))
    act_q = fake_quant(act_t.reshape(features // 16, 16, token_count), 1, act_peak).reshape(
        features, token_count
    )
    weight_q = fake_quant(weight_f.reshape(features // 16, 16, D), 1, weight_peak).reshape(
        features, D
    )
    share_rows = token_count // lax.axis_size("tp")
    projected = lax.psum_scatter(
        lax.dot_general(
            act_q, weight_q, (((0,), (0,)), ((), ())), preferred_element_type=jnp.float32
        ).astype(jnp.bfloat16),
        "tp",
        scatter_dimension=0,
        tiled=True,
    ).astype(jnp.float32)
    hidden_sum = residual.astype(jnp.float32) + projected
    new_residual = hidden_sum.astype(jnp.bfloat16)
    mean_square = jnp.mean(hidden_sum * hidden_sum, axis=1, keepdims=True)
    normed = hidden_sum * lax.rsqrt(mean_square + 1e-05) * norm_gain.astype(jnp.float32)
    norm_peak = lax.pmax(jnp.max(jnp.abs(normed)), ("seq", "tp"))
    next_input = fake_quant(normed.reshape(share_rows, D // 16, 16), 2, norm_peak).reshape(
        share_rows, D
    )
    return (new_residual, next_input)


QB = 16
PIECES = 8
SINE = (0.8999996185302734, -5.921722412109375, 11.687792778015137,
        -10.969291687011719, 5.902237892150879, -1.757728934288025)


def block_factors(block_max, peak):
    tensor_scale = peak / (6.0 * 448.0)
    block_scale = jnp.maximum(block_max / (6.0 * tensor_scale), scale_floor)
    spacing = block_scale.astype(jnp.bfloat16).astype(jnp.float32) * tensor_scale
    return 0.5 / spacing, 2.0 * spacing


def half_payload(t):
    w = t - jnp.round(t)
    z = w * w
    poly = SINE[5]
    for c in SINE[4::-1]:
        poly = poly * z + c
    return (t - w * poly).astype(jnp.bfloat16)


def tree_max16(x):
    rows, lanes = x.shape
    return jnp.max(x.reshape(rows // QB, QB, lanes), axis=1)


def weight_max_kernel(w_ref, bm_ref, top_ref, acc):
    step = pl.program_id(0)
    bm = tree_max16(jnp.abs(w_ref[...]).astype(jnp.float32))
    bm_ref[...] = bm
    part = jnp.max(bm, axis=0, keepdims=True)

    @pl.when(step == 0)
    def _():
        acc[...] = part

    @pl.when(step > 0)
    def _():
        acc[...] = jnp.maximum(acc[...], part)

    @pl.when(step == pl.num_programs(0) - 1)
    def _():
        top_ref[...] = jnp.max(acc[...], axis=1, keepdims=True)


def weight_max(w):
    rows, cols = w.shape
    width = cols // PIECES
    return pl.pallas_call(
        weight_max_kernel,
        grid=(PIECES,),
        in_specs=[pl.BlockSpec((rows, width), lambda i: (0, i))],
        out_specs=[pl.BlockSpec((rows // QB, width), lambda i: (0, i)),
                   pl.BlockSpec((1, 1), lambda i: (0, 0))],
        out_shape=[jax.ShapeDtypeStruct((rows // QB, cols), jnp.float32),
                   jax.ShapeDtypeStruct((1, 1), jnp.float32)],
        scratch_shapes=[pltpu.VMEM((1, width), jnp.float32)],
        cost_estimate=pl.CostEstimate(flops=int(3.2e9), bytes_accessed=rows * cols * 2, transcendentals=0),
        name="weight_max",
    )(w)


def weight_quant_kernel(order_ref, peak_ref, w_ref, bm_ref, out_ref, inv_s, spc_s, q_s):
    inv, spc = block_factors(bm_ref[...], peak_ref[...])
    inv_s[...] = inv
    spc_s[...] = spc
    rows, width = w_ref.shape
    for b in range(rows // QB):
        x = w_ref[pl.ds(b * QB, QB), :].astype(jnp.float32)
        pay = half_payload(x * inv_s[pl.ds(b, 1), :])
        q = (pay.astype(jnp.float32) * spc_s[pl.ds(b, 1), :]).astype(jnp.bfloat16)
        q_s[pl.ds(b * QB, QB), :] = q
    out_ref[...] = q_s[...].T


def weight_quant(order, peak, w, bm, first, count, name):
    rows, cols = w.shape
    width = cols // PIECES
    return pl.pallas_call(
        weight_quant_kernel,
        grid_spec=pltpu.PrefetchScalarGridSpec(
            num_scalar_prefetch=1,
            grid=(count,),
            in_specs=[pl.BlockSpec((1, 1), lambda i, o: (0, 0)),
                      pl.BlockSpec((rows, width), lambda i, o: (0, o[first + i])),
                      pl.BlockSpec((rows // QB, width), lambda i, o: (0, o[first + i]))],
            out_specs=pl.BlockSpec((width, rows), lambda i, o: (i, 0)),
            scratch_shapes=[pltpu.VMEM((rows // QB, width), jnp.float32),
                            pltpu.VMEM((rows // QB, width), jnp.float32),
                            pltpu.VMEM((rows, width), jnp.bfloat16)]),
        out_shape=jax.ShapeDtypeStruct((count * width, rows), jnp.bfloat16),
        cost_estimate=pl.CostEstimate(flops=int(2e9) * count, bytes_accessed=4 * rows * width * count, transcendentals=0),
        name=name,
    )(order, peak, w, bm)


def attention_kernel(pos_ref, q_ref, *refs):
    blocks = len(refs) - 6
    kv_refs = refs[:blocks]
    own_ref, send_ref, top_ref, m_s, l_s, acc_s = refs[blocks:]
    head = pl.program_id(0)
    seq_rank = pos_ref[0]
    tp_rank = pos_ref[1]
    tokens = q_ref.shape[0]
    share = own_ref.shape[1]
    c = HEAD_SIZE ** (-0.5) * math.log2(math.e)

    def scores(kv_ref):
        return lax.dot_general(kv_ref[:, :HEAD_SIZE], q_ref[...], (((1,), (1,)), ((), ())),
                               preferred_element_type=jnp.float32)

    def weighted(kv_ref, p):
        return lax.dot_general(kv_ref[:, HEAD_SIZE:], p.astype(jnp.bfloat16), (((0,), (0,)), ((), ())),
                               preferred_element_type=jnp.float32)

    s = scores(kv_refs[0])
    key_pos = lax.broadcasted_iota(jnp.int32, s.shape, 0)
    query_pos = lax.broadcasted_iota(jnp.int32, s.shape, 1)
    s = jnp.where(key_pos <= query_pos, s, neg_large)
    top = jnp.max(s, axis=0, keepdims=True)
    p = jnp.exp2((s - top) * c)
    m_s[...] = top
    l_s[...] = jnp.sum(p, axis=0, keepdims=True)
    acc_s[...] = weighted(kv_refs[0], p)

    for d in range(1, blocks):
        @pl.when(seq_rank >= d)
        def _(d=d):
            s = scores(kv_refs[d])
            old = m_s[...]
            top = jnp.maximum(old, jnp.max(s, axis=0, keepdims=True))
            p = jnp.exp2((s - top) * c)
            shrink = jnp.exp2((old - top) * c)
            m_s[...] = top
            l_s[...] = l_s[...] * shrink + jnp.sum(p, axis=0, keepdims=True)
            acc_s[...] = acc_s[...] * shrink + weighted(kv_refs[d], p)

    att = (acc_s[...] / l_s[...]).astype(jnp.bfloat16).astype(jnp.float32)
    acc_s[...] = att
    top = jnp.max(jnp.max(jnp.abs(att), axis=0, keepdims=True), axis=1, keepdims=True)

    @pl.when(head == 0)
    def _():
        top_ref[...] = top

    @pl.when(head > 0)
    def _():
        top_ref[...] = jnp.maximum(top_ref[...], top)

    own_ref[...] = acc_s[:, pl.ds(pl.multiple_of(tp_rank * share, share), share)].astype(jnp.bfloat16)
    send_ref[...] = acc_s[:, pl.ds(pl.multiple_of((1 - tp_rank) * share, share), share)].astype(jnp.bfloat16)


def attention(pos, queries, kv_blocks):
    tokens, features = queries.shape
    share = tokens // 2
    heads = features // HEAD_SIZE
    kv_spec = pl.BlockSpec(kv_blocks[0].shape, lambda h, p: (0, 0))
    return pl.pallas_call(
        attention_kernel,
        grid_spec=pltpu.PrefetchScalarGridSpec(
            num_scalar_prefetch=1,
            grid=(heads,),
            in_specs=[pl.BlockSpec((tokens, HEAD_SIZE), lambda h, p: (0, h))] + [kv_spec] * len(kv_blocks),
            out_specs=[pl.BlockSpec((HEAD_SIZE, share), lambda h, p: (h, 0)),
                       pl.BlockSpec((HEAD_SIZE, share), lambda h, p: (h, 0)),
                       pl.BlockSpec((1, 1), lambda h, p: (0, 0))],
            scratch_shapes=[pltpu.VMEM((1, tokens), jnp.float32),
                            pltpu.VMEM((1, tokens), jnp.float32),
                            pltpu.VMEM((HEAD_SIZE, tokens), jnp.float32)]),
        out_shape=[jax.ShapeDtypeStruct((features, share), jnp.bfloat16),
                   jax.ShapeDtypeStruct((features, share), jnp.bfloat16),
                   jax.ShapeDtypeStruct((1, 1), jnp.float32)],
        cost_estimate=pl.CostEstimate(flops=int(8e9), bytes_accessed=3 << 20, transcendentals=0),
        name="attention",
    )(pos, queries, *kv_blocks)


def quant_rows(x, peak):
    rows, lanes = x.shape
    x = x.astype(jnp.float32)
    inv, spc = block_factors(tree_max16(jnp.abs(x)), peak)
    x = x.reshape(rows // QB, QB, lanes)
    pay = half_payload(x * inv[:, None, :])
    q = (pay.astype(jnp.float32) * spc[:, None, :]).astype(jnp.bfloat16)
    return q.reshape(rows, lanes)


def first_half_kernel(order_ref, peak_ref, att_ref, a0_ref, a1_ref, a2_ref, res_ref, out_ref, act_s):
    step = pl.program_id(0)

    @pl.when(step == 0)
    def _():
        act_s[...] = quant_rows(att_ref[...], peak_ref[...])

    def emit(w_ref):
        part = jnp.dot(w_ref[...], act_s[...], preferred_element_type=jnp.float32)
        out_ref[...] = res_ref[...].T.astype(jnp.float32) + part.astype(jnp.bfloat16).astype(jnp.float32)

    @pl.when(step == 0)
    def _():
        emit(a0_ref)

    @pl.when(step == 1)
    def _():
        emit(a1_ref)

    @pl.when(step > 1)
    def _():
        emit(a2_ref)


def first_half(order, peak, att, a0, a1, a2, residual):
    share, cols = residual.shape
    features = att.shape[0]
    width = cols // PIECES
    return pl.pallas_call(
        first_half_kernel,
        grid_spec=pltpu.PrefetchScalarGridSpec(
            num_scalar_prefetch=1,
            grid=(PIECES,),
            in_specs=[pl.BlockSpec((1, 1), lambda i, o: (0, 0)),
                      pl.BlockSpec((features, share), lambda i, o: (0, 0)),
                      pl.BlockSpec((width, features), lambda i, o: (0, 0)),
                      pl.BlockSpec((width, features), lambda i, o: (0, 0)),
                      pl.BlockSpec((width, features), lambda i, o: (jnp.maximum(i - 2, 0), 0)),
                      pl.BlockSpec((share, width), lambda i, o: (0, o[i]))],
            out_specs=pl.BlockSpec((width, share), lambda i, o: (i, 0)),
            scratch_shapes=[pltpu.VMEM((features, share), jnp.bfloat16)]),
        out_shape=jax.ShapeDtypeStruct((cols, share), jnp.float32),
        cost_estimate=pl.CostEstimate(flops=2 * features * share * cols, bytes_accessed=20 << 20, transcendentals=0),
        name="first_half",
    )(order, peak, att, a0, a1, a2, residual)


def second_half_kernel(order_ref, peak_ref, att_ref, h_ref, gain_ref, *refs):
    w_refs = refs[:PIECES]
    res_ref, hg_ref, bm_ref, rstd_ref, top_ref, act_s, w_s, sem, sq_s, run_s = refs[PIECES:]
    step = pl.program_id(0)
    cols = PIECES * h_ref.shape[0]

    def fetch(j):
        return pltpu.make_async_copy(w_refs[j], w_s.at[j], sem.at[j])

    @pl.when(step == 0)
    def _():
        for j in range(PIECES):
            fetch(j).start()
        act_s[...] = quant_rows(att_ref[...], peak_ref[...])

    for j in range(PIECES):
        @pl.when(step == j)
        def _(j=j):
            fetch(j).wait()

    part = jnp.dot(w_s[step], act_s[...], preferred_element_type=jnp.float32)
    h = h_ref[...] + part.astype(jnp.bfloat16).astype(jnp.float32)
    res_ref[...] = h.astype(jnp.bfloat16).T
    sq = jnp.sum(h * h, axis=0, keepdims=True)
    hg = h * gain_ref[...]
    hg_ref[...] = hg
    bm = tree_max16(jnp.abs(hg))
    bm_ref[...] = bm
    run = jnp.max(bm, axis=0, keepdims=True)

    @pl.when(step == 0)
    def _():
        sq_s[...] = sq
        run_s[...] = run

    @pl.when(step > 0)
    def _():
        sq_s[...] = sq_s[...] + sq
        run_s[...] = jnp.maximum(run_s[...], run)

    @pl.when(step == pl.num_programs(0) - 1)
    def _():
        rstd = lax.rsqrt(sq_s[...] / cols + 1e-05)
        rstd_ref[...] = rstd
        top_ref[...] = jnp.max(run_s[...] * rstd, axis=1, keepdims=True)


def second_half(order, peak, att, h, gain, pieces):
    cols, share = h.shape
    features = att.shape[0]
    width = cols // PIECES
    return pl.pallas_call(
        second_half_kernel,
        grid_spec=pltpu.PrefetchScalarGridSpec(
            num_scalar_prefetch=1,
            grid=(PIECES,),
            in_specs=[pl.BlockSpec((1, 1), lambda i, o: (0, 0)),
                      pl.BlockSpec((features, share), lambda i, o: (0, 0)),
                      pl.BlockSpec((width, share), lambda i, o: (i, 0)),
                      pl.BlockSpec((width, 1), lambda i, o: (o[i], 0))]
            + [pl.BlockSpec(memory_space=pl.ANY)] * PIECES,
            out_specs=[pl.BlockSpec((share, width), lambda i, o: (0, o[i])),
                       pl.BlockSpec((width, share), lambda i, o: (i, 0)),
                       pl.BlockSpec((width // QB, share), lambda i, o: (i, 0)),
                       pl.BlockSpec((1, share), lambda i, o: (0, 0)),
                       pl.BlockSpec((1, 1), lambda i, o: (0, 0))],
            scratch_shapes=[pltpu.VMEM((features, share), jnp.bfloat16),
                            pltpu.VMEM((PIECES, width, features), jnp.bfloat16),
                            pltpu.SemaphoreType.DMA((PIECES,)),
                            pltpu.VMEM((1, share), jnp.float32),
                            pltpu.VMEM((1, share), jnp.float32)]),
        out_shape=[jax.ShapeDtypeStruct((share, cols), jnp.bfloat16),
                   jax.ShapeDtypeStruct((cols, share), jnp.float32),
                   jax.ShapeDtypeStruct((cols // QB, share), jnp.float32),
                   jax.ShapeDtypeStruct((1, share), jnp.float32),
                   jax.ShapeDtypeStruct((1, 1), jnp.float32)],
        cost_estimate=pl.CostEstimate(flops=2 * features * share * cols, bytes_accessed=28 << 20, transcendentals=0),
        name="second_half",
    )(order, peak, att, h, gain, *pieces)


def last_quant_kernel(order_ref, peak_ref, rstd_ref, hg_ref, bm_ref, out_ref, inv_s, spc_s):
    rstd = rstd_ref[...]
    inv, spc = block_factors(bm_ref[...] * rstd, peak_ref[...])
    inv_s[...] = inv * rstd
    spc_s[...] = spc
    width, share = hg_ref.shape
    group = 8 * QB
    for g in range(width // group):
        rows = []
        for b in range(g * 8, g * 8 + 8):
            pay = half_payload(hg_ref[pl.ds(b * QB, QB), :] * inv_s[pl.ds(b, 1), :])
            rows.append((pay.astype(jnp.float32) * spc_s[pl.ds(b, 1), :]).astype(jnp.bfloat16))
        out_ref[:, pl.ds(g * group, group)] = jnp.concatenate(rows, axis=0).T


def last_quant(order, peak, rstd, hg, bm):
    cols, share = hg.shape
    width = cols // PIECES
    return pl.pallas_call(
        last_quant_kernel,
        grid_spec=pltpu.PrefetchScalarGridSpec(
            num_scalar_prefetch=1,
            grid=(PIECES,),
            in_specs=[pl.BlockSpec((1, 1), lambda i, o: (0, 0)),
                      pl.BlockSpec((1, share), lambda i, o: (0, 0)),
                      pl.BlockSpec((width, share), lambda i, o: (i, 0)),
                      pl.BlockSpec((width // QB, share), lambda i, o: (i, 0))],
            out_specs=pl.BlockSpec((share, width), lambda i, o: (0, o[i])),
            scratch_shapes=[pltpu.VMEM((width // QB, share), jnp.float32),
                            pltpu.VMEM((width // QB, share), jnp.float32)]),
        out_shape=jax.ShapeDtypeStruct((share, cols), jnp.bfloat16),
        cost_estimate=pl.CostEstimate(flops=int(1e9), bytes_accessed=12 << 20, transcendentals=0),
        name="last_quant",
    )(order, peak, rstd, hg, bm)


def xor_pairs(n, k):
    return [(i, i ^ k) for i in range(n)]


def gather_local(queries, keys, values, out_weight, residual, norm_gain):
    seq_size, dp_size = lax.axis_size("seq"), lax.axis_size("dp")
    seq_rank, dp_rank, tp_rank = lax.axis_index("seq"), lax.axis_index("dp"), lax.axis_index("tp")
    core = seq_rank % 2
    corner = (seq_rank // 2) % 2 + 2 * (dp_rank % 2)
    flips = (0, 3, 1, 2)
    order = jnp.stack([side * 4 + (corner ^ f) for side in (core, 1 - core) for f in flips]).astype(jnp.int32)

    def to_tp(x):
        return lax.ppermute(x, "tp", xor_pairs(2, 1))

    def to_seq(x, k):
        return lax.ppermute(x, "seq", xor_pairs(seq_size, k))

    def to_dp(x):
        return lax.ppermute(x, "dp", xor_pairs(dp_size, 1))

    kv = jnp.concatenate((keys, values), axis=1)
    kv_blocks = [kv] + [
        lax.ppermute(kv, "seq", [(i, i + d) for i in range(seq_size - d)]) for d in range(1, seq_size)
    ]

    bm, weight_top = weight_max(out_weight)
    weight_peak = jnp.maximum(weight_top, to_tp(weight_top))
    a0 = weight_quant(order, weight_peak, out_weight, bm, 0, 1, "quant_0")
    x0 = to_tp(a0)
    a1 = weight_quant(order, weight_peak, out_weight, bm, 1, 1, "quant_1")
    x1 = to_tp(a1)
    a2 = weight_quant(order, weight_peak, out_weight, bm, 2, PIECES - 2, "quant_2")
    x2 = to_seq(x0, 2)
    x3 = to_dp(x0)
    pieces = [x0, x1, x2, x3] + [to_seq(x, 1) for x in (x0, x1, x2, x3)]

    pos = jnp.stack([seq_rank, tp_rank]).astype(jnp.int32)
    att_own, att_send, act_top = attention(pos, queries, kv_blocks)
    att_other = to_tp(att_send)
    act_top = jnp.maximum(act_top, to_seq(act_top, 1))
    act_top = jnp.maximum(act_top, to_seq(act_top, 2))
    act_peak = jnp.maximum(act_top, to_tp(act_top))

    h = first_half(order, act_peak, att_own, a0, a1, a2, residual)
    gain = norm_gain.astype(jnp.float32).reshape(-1, 1)
    new_residual, hg, hbm, rstd, top = second_half(order, act_peak, att_other, h, gain, pieces)
    top = jnp.maximum(top, to_seq(top, 1))
    top = jnp.maximum(top, to_seq(top, 2))
    norm_peak = jnp.maximum(top, to_tp(top))
    next_input = last_quant(order, norm_peak, rstd, hg, hbm)
    return (new_residual, next_input)


def solution(mesh):
    tokens = ("dp", "seq", "tp")
    in_specs = (
        P(("dp", "seq"), "tp"),
        P(("dp", "seq"), "tp"),
        P(("dp", "seq"), "tp"),
        P("tp", None),
        P(tokens, None),
        P(),
    )
    out_specs = (P(tokens, None), P(tokens, None))
    square = mesh.shape["tp"] == 2 and mesh.shape["seq"] == 4 and mesh.shape["dp"] % 2 == 0
    body = gather_local if square else scatter_local
    return jax.shard_map(body, mesh=mesh, in_specs=in_specs, out_specs=out_specs, check_vma=False)
```
